32 devices in a mesh: dp: 8 (over z, core), expert: 4 (over y, x).
Axes of the slice: x: 2, y: 2, z: 4, core: 2. Of those that a mesh axis runs over, the one named last changes fastest.
Arguments:
- tokens: bfloat16 [16384, 2048], P(('dp', 'expert')), parts along dimension 0, may hold values from -6 to 6
- modality: int32 [16384], P(('dp', 'expert')), parts along dimension 0, may hold values 0 or 1
- expert_ids: int32 [16384, 2], P(('dp', 'expert')), parts along dimension 0, may hold values from 0 to 3, all different within a row; in each aligned block of 512 rows (0 to 511, 512 to 1023, ...) at most 320 rows name the same one
- route_weights: float32 [16384, 2], P(('dp', 'expert')), parts along dimension 0, may hold values from 0.25 to 1
- norm_gain: float32 [2, 2048], replicated, may hold values from 0.25 to 1.75
- gate_weight: bfloat16 [2048, 3584], P(None, 'expert'), may hold values from -0.125 to 0.125
- up_weight: bfloat16 [2048, 3584], P(None, 'expert'), may hold values from -0.125 to 0.125
- down_weight: bfloat16 [3584, 2048], P('expert'), may hold values from -0.1875 to 0.1875
Outputs:
- mixed: bfloat16 [16384, 2048], P(('dp', 'expert')), parts along dimension 0
The draws below stay inside these ranges and needn't reach their ends.
There are 8 independent parts, one for each index of `dp`. The reference program is written for one: setup_inputs(seed, part) draws one part's arguments, and reference() takes and returns one part's arrays. A program takes and returns all parts, laid end to end along the dimension named above; an argument that names none is the same for every part. Nothing has to cross between parts.
Inputs may be any that keep to these rules, and one draw needn't show every extreme that they name: `expert_ids`: each row names 2 different experts. Among the rows of one device no expert is named by more than 320 rows, a bound that some blocks reach.
All inputs are finite; a program needn't handle non-finite values. No bound on the sum of `modality` on one device may be relied on, other than what follows from the above.
Results may differ from the reference program's by a relative error of at most 0.0054.
Values may be sent and summed in bfloat16 or wider, within the bound.
No kernel may reach another device: no remote copies, remote signals or barrier semaphores. Data moves between devices by JAX's collectives and lax.ppermute only.
A program may use at most 128 MiB of HBM per device.

```python
import math
import jax
import jax.numpy as jnp
import numpy as np
from jax import lax

D = 2048
HIDDEN_SIZE = 896
TOP = 2
TOK_DEV = 512
EXPERTS = 4
CAP = 320
TOKENS = 2048
N_EXPERT = 4


def set_ends(result, stream_key, low, largest):
    dims = result.shape
    index_at = [jax.random.randint(jax.random.fold_in(stream_key, axis), (), 0, dims[axis]) for axis in range(len(dims))]
    result = result.at[tuple(index_at)].set(low)
    longest = dims.index(max(dims))
    index_at[longest] = (index_at[longest] + 1) % dims[longest]
    return result.at[tuple(index_at)].set(largest)


def block_scale(own_key, shape, shards, least, high):
    def one(dim, shards_of):
        steps = jax.random.uniform(jax.random.fold_in(jax.random.fold_in(own_key, 6), dim), (shards_of,), jnp.float32, least / len(shards), high / len(shards))
        return jnp.repeat(jnp.exp(steps), shape[dim] // shards_of).reshape((-1,) + (1,) * (len(shape) - dim - 1))

    gain = one(*shards[0])
    for cut in shards[1:]:
        gain = gain * one(*cut)
    return gain


def deal_out(key, own, number, rows, count, top, limit, lean):
    order = jax.random.permutation(key, count)
    heavy_load, ordinary = shares(count, rows * top, limit, lean, True), shares(count, rows * top, limit, lean, False)
    places = jnp.arange(count)

    def named(sizes, offset_by):
        used = int((sizes > 0).sum())
        fixed = max(1, used // 4)
        moved = fixed + (places - fixed + offset_by * (used - fixed)) % max(1, count - fixed)
        return jnp.zeros((count,), jnp.int32).at[order[jnp.where(places < fixed, places, moved)]].set(jnp.asarray(sizes, jnp.int32))

    sizes = jnp.where(number % 4 == 0, named(heavy_load, number // 4), named(ordinary, number - number // 4 - 1))
    mixed = jax.random.permutation(jax.random.fold_in(own, 3), count)
    source_of, taker = mixed[0:count // 2 * 2:2], mixed[1:count // 2 * 2:2]
    room = jnp.minimum(sizes[source_of] - 1, limit - sizes[taker]) // 2
    room = jnp.where((source_of == order[0]) | (taker == order[0]) | (sizes[taker] == 0), 0, jnp.maximum(room, 0))
    moved = jax.random.randint(jax.random.fold_in(own, 4), (count // 2,), 0, 1 << 20) % (room + 1)
    sizes = sizes.at[source_of].add(-moved).at[taker].add(moved)
    labels = jnp.searchsorted(jnp.cumsum(sizes), jnp.arange(rows * top), side="right").astype(jnp.int32)
    table = labels.reshape(top, rows).T
    table = table[jax.random.permutation(jax.random.fold_in(own, 1), rows)]
    offset_by = jax.random.randint(jax.random.fold_in(own, 2), (rows, 1), 0, top)
    return jnp.take_along_axis(table, (jnp.arange(top)[None, :] + offset_by) % top, axis=1)


def shares(number_of, total, bound, slope, full):
    loads = [(1 << 20) // math.isqrt(rank ** slope) + 1 for rank in range(1, number_of + 1)]
    largest = bound if full else min(bound, max(-(-total // number_of), total * loads[0] // sum(loads)))
    least = 1 if total - largest >= number_of - 1 else 0
    counts, rest = [largest] + [least] * (number_of - 1), total - largest - least * (number_of - 1)
    while rest > 0:
        free = [i for i in range(1, number_of) if counts[i] < largest] or [i for i in range(1, number_of) if counts[i] < bound]
        pool, budget = sum([loads[i] for i in free]), rest
        for i in free:
            extra = min(bound - counts[i], max(1, budget * loads[i] // pool), rest)
            counts[i] = counts[i] + extra
            rest = rest - extra
    return np.array(counts)


def bell_draw(stream_key, shape, spread, most, split=(), held_as=jnp.bfloat16):
    factor_of = block_scale(stream_key, shape, split, -0.22, 0.18) if split else 1.0
    result = jax.random.normal(stream_key, shape, jnp.float32) * spread * factor_of
    return jnp.minimum(jnp.maximum(result, -most), most).astype(held_as)


def setup_inputs(seed: int = 0, part: int = 0) -> dict:
    key_list = jax.random.split(jax.random.key(seed), 9)
    part_splits = jax.random.split(jax.random.fold_in(key_list[8], part), 9)
    tokens = bell_draw(part_splits[0], (TOKENS, D), 1.0, 6.0, ((0, 4),))
    modality = set_ends((jax.random.randint(part_splits[1], (TOKENS,), 0, 2) < 1).astype(jnp.int32), jax.random.fold_in(part_splits[1], 1), 0, 1)
    expert_ids_keys = jax.random.split(jax.random.fold_in(part_splits[2], 1), TOKENS // TOK_DEV)
    expert_ids_turns = jax.random.permutation(jax.random.fold_in(part_splits[2], 3), TOKENS // TOK_DEV)
    expert_ids = jax.vmap(lambda own, number: deal_out(jax.random.fold_in(part_splits[2], 2), own, number, TOK_DEV, EXPERTS, TOP, CAP, 1))(expert_ids_keys, expert_ids_turns).reshape((TOKENS, TOP))
    route_weights = jnp.clip(0.25 + 0.75 * jax.random.uniform(part_splits[3], (TOKENS, TOP), jnp.float32) ** block_scale(part_splits[3], (TOKENS, TOP), ((0, 4),), -0.2, 0.2), 0.25, 1.0)
    norm_gain = jnp.clip(1.0 + 0.15 * jax.random.normal(key_list[4], (2, D), jnp.float32), 0.25, 1.75)
    gate_weight = bell_draw(key_list[5], (D, EXPERTS * HIDDEN_SIZE), D ** -0.5, 0.125, ((1, 4),))
    up_weight = bell_draw(key_list[6], (D, EXPERTS * HIDDEN_SIZE), D ** -0.5, 0.125, ((1, 4),))
    down_weight = bell_draw(key_list[7], (EXPERTS * HIDDEN_SIZE, D), HIDDEN_SIZE ** -0.5, 0.1875, ((0, 4),))
    return dict(tokens=tokens, modality=modality, expert_ids=expert_ids, route_weights=route_weights, norm_gain=norm_gain, gate_weight=gate_weight, up_weight=up_weight, down_weight=down_weight)


epsilon = 1e-05

def normalize(tokens, modality, norm_gain):
    values = tokens.astype(jnp.float32)
    square = lax.optimization_barrier(jnp.mean(values * values, axis=1, keepdims=True))
    gains = jnp.where(modality[:, None] == 1, norm_gain[1][None, :], norm_gain[0][None, :])
    return (values * lax.rsqrt(square + epsilon) * gains).astype(jnp.bfloat16)

def slot_table(expert_ids, experts, capacity):
    fanout = expert_ids.shape[1]
    flat_ids = expert_ids.reshape(-1).astype(jnp.int32)
    columns = jnp.arange(experts, dtype=jnp.int32)
    onehot = (flat_ids[:, None] == columns[None, :]).astype(jnp.int32)
    earlier = jnp.cumsum(onehot, axis=0).astype(jnp.int32) - onehot
    position = lax.optimization_barrier(jnp.sum(earlier * onehot, axis=1)).astype(jnp.int32)
    slots = (flat_ids * capacity + position).astype(jnp.int32)
    sources = (jnp.arange(flat_ids.shape[0], dtype=jnp.int32) // fanout).astype(jnp.int32)
    owners = jnp.full((experts * capacity,), -1, jnp.int32).at[slots].set(sources)
    return (slots, owners)

def pack_rows(normed, owners):
    chosen = jnp.take(normed, jnp.maximum(owners, 0), axis=0)
    return jnp.where(owners[:, None] >= 0, chosen, jnp.zeros_like(chosen))

def expert_rows(rows, gate_cols, up_cols, down_rows):
    gate = jnp.dot(rows, gate_cols, preferred_element_type=jnp.float32)
    upper = jnp.dot(rows, up_cols, preferred_element_type=jnp.float32)
    active = (jax.nn.silu(gate) * upper).astype(jnp.bfloat16)
    return jnp.dot(active, down_rows, preferred_element_type=jnp.float32)

def reference(tokens, modality, expert_ids, route_weights, norm_gain, gate_weight, up_weight, down_weight):
    normed = normalize(tokens, modality, norm_gain)
    block_normed = normed.reshape(N_EXPERT, TOK_DEV, D)
    block_ids = expert_ids.reshape(N_EXPERT, TOK_DEV, TOP)
    slots, owners = jax.vmap(lambda ids: slot_table(ids, EXPERTS, CAP))(block_ids)
    packed = jax.vmap(pack_rows)(block_normed, owners)
    per_expert = packed.reshape(N_EXPERT, EXPERTS, CAP, D).transpose(1, 0, 2, 3).reshape(EXPERTS, N_EXPERT * CAP, D)

    def run_one(index):
        start = (index * HIDDEN_SIZE).astype(jnp.int32)
        gate_cols = lax.dynamic_slice_in_dim(gate_weight, start, HIDDEN_SIZE, 1)
        up_cols = lax.dynamic_slice_in_dim(up_weight, start, HIDDEN_SIZE, 1)
        down_rows = lax.dynamic_slice_in_dim(down_weight, start, HIDDEN_SIZE, 0)
        rows = lax.dynamic_index_in_dim(per_expert, index, 0, keepdims=False)
        return expert_rows(rows, gate_cols, up_cols, down_rows).astype(jnp.bfloat16)
    outputs = lax.map(run_one, jnp.arange(EXPERTS, dtype=jnp.int32))
    by_block = outputs.reshape(EXPERTS, N_EXPERT, CAP, D).transpose(1, 0, 2, 3).reshape(N_EXPERT, EXPERTS * CAP, D)
    picked = jax.vmap(lambda table, where_to: jnp.take(table, where_to, axis=0))(by_block, slots)
    picked = picked.reshape(TOKENS, TOP, D).astype(jnp.float32)
    mixed = tokens.astype(jnp.float32) + lax.optimization_barrier(jnp.sum(route_weights[:, :, None] * picked, axis=1))
    return mixed.astype(jnp.bfloat16)
```

```python
import functools
import jax
import jax.numpy as jnp
from jax import lax
from jax.experimental import pallas as pl
from jax.experimental.pallas import tpu as pltpu
from jax.sharding import PartitionSpec as P


epsilon = 1e-05
SMEM = pltpu.MemorySpace.SMEM


def normalize(tokens, modality, norm_gain):
    values = tokens.astype(jnp.float32)
    square = jnp.mean(values * values, axis=1, keepdims=True)
    gains = jnp.where(modality[:, None] == 1, norm_gain[1][None, :], norm_gain[0][None, :])
    return (values * lax.rsqrt(square + epsilon) * gains).astype(jnp.bfloat16)


def slot_table(expert_ids, experts, capacity):
    fanout = expert_ids.shape[1]
    flat_ids = expert_ids.reshape(-1)
    columns = jnp.arange(experts, dtype=jnp.int32)
    onehot = (flat_ids[:, None] == columns[None, :]).astype(jnp.int32)
    earlier = jnp.cumsum(onehot, axis=0) - onehot
    position = jnp.sum(earlier * onehot, axis=1)
    slots = flat_ids * capacity + position
    sources = jnp.arange(flat_ids.shape[0], dtype=jnp.int32) // fanout
    owners = jnp.full((experts * capacity,), -1, jnp.int32).at[slots].set(sources)
    return (slots, owners)


def pack_rows(normed, owners):
    chosen = jnp.take(normed, jnp.maximum(owners, 0), axis=0)
    return jnp.where(owners[:, None] >= 0, chosen, jnp.zeros_like(chosen))


def expert_rows(rows, gate_weight, up_weight, down_weight):
    gate = jnp.dot(rows, gate_weight, preferred_element_type=jnp.float32)
    upper = jnp.dot(rows, up_weight, preferred_element_type=jnp.float32)
    active = (jax.nn.silu(gate) * upper).astype(jnp.bfloat16)
    return jnp.dot(active, down_weight, preferred_element_type=jnp.float32).astype(jnp.bfloat16)


def general(
    tokens, modality, expert_ids, route_weights, norm_gain, gate_weight, up_weight, down_weight
):
    devices = lax.axis_size("expert")
    tok_rows, width = tokens.shape
    fanout = expert_ids.shape[1]
    capacity = min(tok_rows, tok_rows * fanout * 5 // (4 * devices))
    normed = normalize(tokens, modality, norm_gain)
    slots, owners = slot_table(expert_ids, devices, capacity)
    blocks = pack_rows(normed, owners).reshape(devices, capacity, width)
    arrived = lax.all_to_all(blocks, "expert", split_axis=0, concat_axis=0, tiled=True)
    finished = expert_rows(
        arrived.reshape(-1, width), gate_weight, up_weight, down_weight
    ).reshape(devices, capacity, width)
    returned = lax.all_to_all(finished, "expert", split_axis=0, concat_axis=0, tiled=True)
    expert_out = returned.reshape(devices * capacity, width)
    picked = (
        jnp.take(expert_out, slots, axis=0).reshape(tok_rows, fanout, width).astype(jnp.float32)
    )
    mixed = tokens.astype(jnp.float32) + jnp.sum(route_weights[:, :, None] * picked, axis=1)
    return mixed.astype(jnp.bfloat16)


def slot_rows(slot_of, first, rows):
    want = lax.broadcasted_iota(jnp.int32, (rows, slot_of.shape[1]), 0) + first
    return jnp.where(want == slot_of, 1.0, 0.0).astype(jnp.bfloat16)


def first_pack_kernel(
    spans, me_ref, ids_ref, mod_ref, weight_ref, tok_ref, gain_ref, *refs
):
    outs, (copy_ref, slot_ref, meta_ref, select, normed_ref) = refs[: len(spans)], refs[len(spans) :]
    step = pl.program_id(0)
    tok_rows = tok_ref.shape[0]
    cols = outs[0].shape[1]

    @pl.when(step == 0)
    def _():
        ids = ids_ref[...]
        rank = lax.broadcasted_iota(jnp.int32, (8, tok_rows), 0)
        wanted = jnp.bitwise_xor(rank, me_ref[0])
        hit0, hit1 = wanted == ids[0:1, :], wanted == ids[1:2, :]
        member = jnp.where((hit0 | hit1) & (rank < 4), 1.0, 0.0)
        weight = jnp.where(hit0, weight_ref[0:1, :], jnp.where(hit1, weight_ref[1:2, :], 0.0))
        before = lax.broadcasted_iota(jnp.int32, (tok_rows, tok_rows), 0) < lax.broadcasted_iota(
            jnp.int32, (tok_rows, tok_rows), 1
        )
        earlier = jnp.dot(
            member.astype(jnp.bfloat16),
            jnp.where(before, 1.0, 0.0).astype(jnp.bfloat16),
            preferred_element_type=jnp.float32,
        )
        place = jnp.where(member > 0, earlier, -1.0)
        slot_ref[...] = place.astype(jnp.int32)
        packed = jnp.concatenate([place[0:4], weight[0:4]], axis=0)
        meta_ref[...] = jnp.concatenate(
            [packed, jnp.zeros((120, tok_rows), jnp.float32)], axis=0
        ).T
        image = jnp.concatenate(
            [mod_ref[...].astype(jnp.float32), jnp.zeros((127, tok_rows), jnp.float32)], axis=0
        ).T[:, 0:1]
        for lo in range(0, tok_rows, 64):
            values = tok_ref[lo : lo + 64, :].astype(jnp.float32)
            square = jnp.mean(values * values, axis=1, keepdims=True)
            gains = jnp.where(image[lo : lo + 64] > 0.5, gain_ref[1:2, :], gain_ref[0:1, :])
            normed_ref[lo : lo + 64, :] = (
                values * lax.rsqrt(square + epsilon) * gains
            ).astype(jnp.bfloat16)
        base = 0
        for j, first, rows in spans:
            select[base : base + rows, :] = slot_rows(place[j : j + 1, :].astype(jnp.int32), first, rows)
            base += rows

    base = 0
    at = pl.ds(pl.multiple_of(step * cols, cols), cols)
    part = normed_ref[:, at]
    copy_ref[...] = part
    chosen = jnp.dot(select[...], part, preferred_element_type=jnp.float32).astype(jnp.bfloat16)
    for out, (j, first, rows) in zip(outs, spans):
        out[...] = chosen[base : base + rows]
        base += rows


def first_pack(me, ids_t, mod, weight_t, tokens, gain, spans, tiles):
    tok_rows, width = tokens.shape
    cols = width // tiles
    whole = lambda *shape: pl.BlockSpec(shape, lambda i: (0,) * len(shape))
    return pl.pallas_call(
        functools.partial(first_pack_kernel, spans),
        grid=(tiles,),
        in_specs=[
            pl.BlockSpec(memory_space=SMEM),
            whole(*ids_t.shape),
            whole(*mod.shape),
            whole(*weight_t.shape),
            whole(*tokens.shape),
            whole(*gain.shape),
        ],
        out_specs=[pl.BlockSpec((rows, cols), lambda i: (0, i)) for _, _, rows in spans]
        + [pl.BlockSpec((tok_rows, cols), lambda i: (0, i)), whole(8, tok_rows), whole(tok_rows, 128)],
        out_shape=[jax.ShapeDtypeStruct((rows, width), jnp.bfloat16) for _, _, rows in spans]
        + [
            jax.ShapeDtypeStruct((tok_rows, width), jnp.bfloat16),
            jax.ShapeDtypeStruct((8, tok_rows), jnp.int32),
            jax.ShapeDtypeStruct((tok_rows, 128), jnp.float32),
        ],
        scratch_shapes=[
            pltpu.VMEM((sum(s[2] for s in spans), tok_rows), jnp.bfloat16),
            pltpu.VMEM((tok_rows, width), jnp.bfloat16),
        ],
        cost_estimate=pl.CostEstimate(
            flops=2 * sum(s[2] for s in spans) * tok_rows * width,
            bytes_accessed=4 * tok_rows * width * 2,
            transcendentals=0,
        ),
        name="first_pack",
    )(me, ids_t, mod, weight_t, tokens, gain)


def more_pack_kernel(spans, slot_ref, normed_ref, *refs):
    outs, select = refs[:-1], refs[-1]

    @pl.when(pl.program_id(0) == 0)
    def _():
        base = 0
        for j, first, rows in spans:
            select[base : base + rows, :] = slot_rows(slot_ref[j : j + 1, :], first, rows)
            base += rows

    chosen = jnp.dot(select[...], normed_ref[...], preferred_element_type=jnp.float32).astype(jnp.bfloat16)
    base = 0
    for out, (j, first, rows) in zip(outs, spans):
        out[...] = chosen[base : base + rows]
        base += rows


def more_pack(slots, normed, spans, tiles):
    tok_rows, width = normed.shape
    cols = width // tiles
    return pl.pallas_call(
        functools.partial(more_pack_kernel, spans),
        grid=(tiles,),
        in_specs=[
            pl.BlockSpec(slots.shape, lambda i: (0, 0)),
            pl.BlockSpec((tok_rows, cols), lambda i: (0, i)),
        ],
        out_specs=[pl.BlockSpec((rows, cols), lambda i: (0, i)) for _, _, rows in spans],
        out_shape=[jax.ShapeDtypeStruct((rows, width), jnp.bfloat16) for _, _, rows in spans],
        scratch_shapes=[pltpu.VMEM((sum(s[2] for s in spans), tok_rows), jnp.bfloat16)],
        cost_estimate=pl.CostEstimate(
            flops=2 * sum(s[2] for s in spans) * tok_rows * width,
            bytes_accessed=4 * tok_rows * width * 2,
            transcendentals=0,
        ),
        name="more_pack",
    )(slots, normed)


def combine_kernel(spans, meta_ref, base_ref, *refs):
    rows_in, out_ref, (spread, gathered) = refs[: len(spans)], refs[len(spans)], refs[len(spans) + 1 :]

    @pl.when(pl.program_id(0) == 0)
    def _():
        lane = lax.broadcasted_iota(jnp.int32, spread.shape, 1)
        total, at = jnp.zeros(spread.shape, jnp.float32), 0
        for j, first, rows in spans:
            place = meta_ref[:, j : j + 1].astype(jnp.int32)
            inside = (place >= first) & (place < first + rows)
            target = jnp.where(inside, place - first + at, -1)
            total = jnp.where(lane == target, meta_ref[:, 4 + j : 5 + j], total)
            at += rows
        spread[...] = total.astype(jnp.bfloat16)

    at = 0
    for (j, first, rows), ref in zip(spans, rows_in):
        gathered[at : at + rows, :] = ref[...]
        at += rows
    total = base_ref[...].astype(jnp.float32) + jnp.dot(
        spread[...], gathered[...], preferred_element_type=jnp.float32
    )
    out_ref[...] = total.astype(out_ref.dtype)


def combine(meta, base, pieces, spans, tiles, dtype):
    tok_rows, width = base.shape
    cols = width // tiles
    return pl.pallas_call(
        functools.partial(combine_kernel, spans),
        grid=(tiles,),
        in_specs=[
            pl.BlockSpec(meta.shape, lambda i: (0, 0)),
            pl.BlockSpec((tok_rows, cols), lambda i: (0, i)),
        ]
        + [pl.BlockSpec((rows, cols), lambda i: (0, i)) for _, _, rows in spans],
        out_specs=pl.BlockSpec((tok_rows, cols), lambda i: (0, i)),
        out_shape=jax.ShapeDtypeStruct((tok_rows, width), dtype),
        scratch_shapes=[
            pltpu.VMEM((tok_rows, sum(s[2] for s in spans)), jnp.bfloat16),
            pltpu.VMEM((sum(s[2] for s in spans), cols), jnp.bfloat16),
        ],
        cost_estimate=pl.CostEstimate(
            flops=2 * sum(s[2] for s in spans) * tok_rows * width,
            bytes_accessed=4 * tok_rows * width * 2,
            transcendentals=0,
        ),
        name="combine",
    )(meta, base, *pieces)


def square(
    tokens, modality, expert_ids, route_weights, norm_gain, gate_weight, up_weight, down_weight
):
    tok_rows, _ = tokens.shape
    capacity = min(tok_rows, tok_rows * expert_ids.shape[1] * 5 // 16)
    half = capacity // 2
    me = lax.axis_index("expert").astype(jnp.int32).reshape(1)
    swap = lambda value, j: lax.ppermute(value, "expert", [(i, i ^ j) for i in range(4)])
    remote = (1, 2, 3)
    spans0 = tuple((j, 0, half) for j in remote)
    spans1 = tuple((j, half, capacity - half) for j in remote)
    *out0, normed, slots, meta = first_pack(
        me, expert_ids.T, modality[None, :], route_weights.T, tokens, norm_gain, spans0, 4
    )
    got0 = [swap(v, j) for v, j in zip(out0, remote)]
    *out1, local = more_pack(slots, normed, spans1 + ((0, 0, capacity),), 4)
    got1 = [swap(v, j) for v, j in zip(out1, remote)]
    ffn = lambda rows: expert_rows(rows, gate_weight, up_weight, down_weight)
    local_out = ffn(local)
    *got0, local_out = lax.optimization_barrier((*got0, local_out))

    def work(got):
        return ffn(jnp.concatenate(got, axis=0))

    def back(done, sizes):
        pieces, at = [], 0
        for j, n in zip(remote, sizes):
            pieces.append(swap(done[at : at + n], j))
            at += n
        return pieces

    done0 = work(got0)
    ret0 = back(done0, [s[2] for s in spans0])
    *got1, _ = lax.optimization_barrier((*got1, done0))
    ret1 = back(work(got1), [s[2] for s in spans1])
    partial = combine(
        meta, tokens, [local_out] + ret0, ((0, 0, capacity),) + spans0, 4, jnp.float32
    )
    return combine(meta, partial, ret1, spans1, 4, jnp.bfloat16)


def shards(*args):
    return (square if lax.axis_size("expert") == 4 else general)(*args)


def solution(mesh):
    placed = (
        P(("dp", "expert"), None),
        P(("dp", "expert")),
        P(("dp", "expert"), None),
        P(("dp", "expert"), None),
        P(),
        P(None, "expert"),
        P(None, "expert"),
        P("expert", None),
    )
    return jax.shard_map(
        shards, mesh=mesh, in_specs=placed, out_specs=P(("dp", "expert"), None), check_vma=False
    )
```

```python
import functools
import jax
import jax.numpy as jnp
from jax import lax
from jax.experimental import pallas as pl
from jax.experimental.pallas import tpu as pltpu
from jax.sharding import PartitionSpec as P


epsilon = 1e-05
VMEM = pltpu.MemorySpace.VMEM
SMEM = pltpu.MemorySpace.SMEM


def normalize(tokens, modality, norm_gain):
    values = tokens.astype(jnp.float32)
    square = jnp.mean(values * values, axis=1, keepdims=True)
    gains = jnp.where(modality[:, None] == 1, norm_gain[1][None, :], norm_gain[0][None, :])
    return (values * lax.rsqrt(square + epsilon) * gains).astype(jnp.bfloat16)


def slot_table(expert_ids, experts, capacity):
    fanout = expert_ids.shape[1]
    flat_ids = expert_ids.reshape(-1)
    columns = jnp.arange(experts, dtype=jnp.int32)
    onehot = (flat_ids[:, None] == columns[None, :]).astype(jnp.int32)
    earlier = jnp.cumsum(onehot, axis=0) - onehot
    position = jnp.sum(earlier * onehot, axis=1)
    slots = flat_ids * capacity + position
    sources = jnp.arange(flat_ids.shape[0], dtype=jnp.int32) // fanout
    owners = jnp.full((experts * capacity,), -1, jnp.int32).at[slots].set(sources)
    return (slots, owners)


def pack_rows(normed, owners):
    chosen = jnp.take(normed, jnp.maximum(owners, 0), axis=0)
    return jnp.where(owners[:, None] >= 0, chosen, jnp.zeros_like(chosen))


def expert_rows(rows, gate_weight, up_weight, down_weight):
    gate = jnp.dot(rows, gate_weight, preferred_element_type=jnp.float32)
    upper = jnp.dot(rows, up_weight, preferred_element_type=jnp.float32)
    active = (jax.nn.silu(gate) * upper).astype(jnp.bfloat16)
    return jnp.dot(active, down_weight, preferred_element_type=jnp.float32).astype(jnp.bfloat16)


def general(
    tokens, modality, expert_ids, route_weights, norm_gain, gate_weight, up_weight, down_weight
):
    devices = lax.axis_size("expert")
    tok_rows, width = tokens.shape
    fanout = expert_ids.shape[1]
    capacity = min(tok_rows, tok_rows * fanout * 5 // (4 * devices))
    normed = normalize(tokens, modality, norm_gain)
    slots, owners = slot_table(expert_ids, devices, capacity)
    blocks = pack_rows(normed, owners).reshape(devices, capacity, width)
    arrived = lax.all_to_all(blocks, "expert", split_axis=0, concat_axis=0, tiled=True)
    finished = expert_rows(
        arrived.reshape(-1, width), gate_weight, up_weight, down_weight
    ).reshape(devices, capacity, width)
    returned = lax.all_to_all(finished, "expert", split_axis=0, concat_axis=0, tiled=True)
    expert_out = returned.reshape(devices * capacity, width)
    picked = (
        jnp.take(expert_out, slots, axis=0).reshape(tok_rows, fanout, width).astype(jnp.float32)
    )
    mixed = tokens.astype(jnp.float32) + jnp.sum(route_weights[:, :, None] * picked, axis=1)
    return mixed.astype(jnp.bfloat16)


def slot_rows(slot_of, first, rows):
    want = lax.broadcasted_iota(jnp.int32, (rows, slot_of.shape[1]), 0) + first
    return jnp.where(want == slot_of, 1.0, 0.0).astype(jnp.bfloat16)


def first_pack_kernel(
    spans, me_ref, ids_hbm, mod_hbm, weight_hbm, tok_hbm, gain_hbm, *refs
):
    outs, rest = refs[: len(spans)], refs[len(spans) :]
    copy_ref, slot_ref, meta_ref, select, normed_ref = rest[:5]
    ids_ref, mod_ref, weight_ref, tok_ref, gain_ref, sems = rest[5:]
    step = pl.program_id(0)
    tok_rows = tok_ref.shape[0]
    cols = outs[0].shape[1]

    @pl.when(step == 0)
    def _():
        pairs = ((ids_hbm, ids_ref), (mod_hbm, mod_ref), (weight_hbm, weight_ref))
        pairs += ((gain_hbm, gain_ref), (tok_hbm, tok_ref))
        copies = [pltpu.make_async_copy(x, y, sems.at[i]) for i, (x, y) in enumerate(pairs)]
        for c in copies:
            c.start()
        for c in copies[:-1]:
            c.wait()
        ids = ids_ref[...]
        rank = lax.broadcasted_iota(jnp.int32, (8, tok_rows), 0)
        wanted = jnp.bitwise_xor(rank, me_ref[0])
        hit0, hit1 = wanted == ids[0:1, :], wanted == ids[1:2, :]
        member = jnp.where((hit0 | hit1) & (rank < 4), 1.0, 0.0)
        weight = jnp.where(hit0, weight_ref[0:1, :], jnp.where(hit1, weight_ref[1:2, :], 0.0))
        before = lax.broadcasted_iota(jnp.int32, (tok_rows, tok_rows), 0) < lax.broadcasted_iota(
            jnp.int32, (tok_rows, tok_rows), 1
        )
        earlier = jnp.dot(
            member.astype(jnp.bfloat16),
            jnp.where(before, 1.0, 0.0).astype(jnp.bfloat16),
            preferred_element_type=jnp.float32,
        )
        place = jnp.where(member > 0, earlier, -1.0)
        slot_ref[...] = place.astype(jnp.int32)
        packed = jnp.concatenate([place[0:4], weight[0:4]], axis=0)
        meta_ref[...] = jnp.concatenate(
            [packed, jnp.zeros((120, tok_rows), jnp.float32)], axis=0
        ).T
        image = jnp.concatenate(
            [mod_ref[...].astype(jnp.float32), jnp.zeros((127, tok_rows), jnp.float32)], axis=0
        ).T[:, 0:1]
        copies[-1].wait()
        for lo in range(0, tok_rows, 64):
            values = tok_ref[lo : lo + 64, :].astype(jnp.float32)
            square = jnp.mean(values * values, axis=1, keepdims=True)
            gains = jnp.where(image[lo : lo + 64] > 0.5, gain_ref[1:2, :], gain_ref[0:1, :])
            normed_ref[lo : lo + 64, :] = (
                values * lax.rsqrt(square + epsilon) * gains
            ).astype(jnp.bfloat16)
        base = 0
        for j, first, rows in spans:
            select[base : base + rows, :] = slot_rows(place[j : j + 1, :].astype(jnp.int32), first, rows)
            base += rows

    base = 0
    at = pl.ds(pl.multiple_of(step * cols, cols), cols)
    part = normed_ref[:, at]
    copy_ref[...] = part
    chosen = jnp.dot(select[...], part, preferred_element_type=jnp.float32).astype(jnp.bfloat16)
    for out, (j, first, rows) in zip(outs, spans):
        out[...] = chosen[base : base + rows]
        base += rows


def first_pack(me, ids_t, mod, weight_t, tokens, gain, spans, tiles):
    tok_rows, width = tokens.shape
    cols = width // tiles
    whole = lambda *shape: pl.BlockSpec(shape, lambda i: (0,) * len(shape))
    return pl.pallas_call(
        functools.partial(first_pack_kernel, spans),
        grid=(tiles,),
        in_specs=[
            pl.BlockSpec(memory_space=SMEM),
        ]
        + [pl.BlockSpec(memory_space=pltpu.MemorySpace.HBM)] * 5,
        out_specs=[pl.BlockSpec((rows, cols), lambda i: (0, i)) for _, _, rows in spans]
        + [pl.BlockSpec((tok_rows, cols), lambda i: (0, i)), whole(8, tok_rows), whole(tok_rows, 128)],
        out_shape=[jax.ShapeDtypeStruct((rows, width), jnp.bfloat16) for _, _, rows in spans]
        + [
            jax.ShapeDtypeStruct((tok_rows, width), jnp.bfloat16),
            jax.ShapeDtypeStruct((8, tok_rows), jnp.int32),
            jax.ShapeDtypeStruct((tok_rows, 128), jnp.float32),
        ],
        scratch_shapes=[
            pltpu.VMEM((sum(s[2] for s in spans), tok_rows), jnp.bfloat16),
            pltpu.VMEM((tok_rows, width), jnp.bfloat16),
            pltpu.VMEM(ids_t.shape, ids_t.dtype),
            pltpu.VMEM(mod.shape, mod.dtype),
            pltpu.VMEM(weight_t.shape, weight_t.dtype),
            pltpu.VMEM(tokens.shape, tokens.dtype),
            pltpu.VMEM(gain.shape, gain.dtype),
            pltpu.SemaphoreType.DMA((5,)),
        ],
        cost_estimate=pl.CostEstimate(
            flops=2 * sum(s[2] for s in spans) * tok_rows * width,
            bytes_accessed=4 * tok_rows * width * 2,
            transcendentals=0,
        ),
        compiler_params=pltpu.CompilerParams(vmem_limit_bytes=16 << 20),
        name="first_pack",
    )(me, ids_t, mod, weight_t, tokens, gain)


def more_pack_kernel(spans, slot_ref, normed_ref, *refs):
    outs, select = refs[:-1], refs[-1]

    @pl.when(pl.program_id(0) == 0)
    def _():
        base = 0
        for j, first, rows in spans:
            select[base : base + rows, :] = slot_rows(slot_ref[j : j + 1, :], first, rows)
            base += rows

    chosen = jnp.dot(select[...], normed_ref[...], preferred_element_type=jnp.float32).astype(jnp.bfloat16)
    base = 0
    for out, (j, first, rows) in zip(outs, spans):
        out[...] = chosen[base : base + rows]
        base += rows


def more_pack(slots, normed, spans, tiles):
    tok_rows, width = normed.shape
    cols = width // tiles
    return pl.pallas_call(
        functools.partial(more_pack_kernel, spans),
        grid=(tiles,),
        in_specs=[
            pl.BlockSpec(slots.shape, lambda i: (0, 0)),
            pl.BlockSpec((tok_rows, cols), lambda i: (0, i)),
        ],
        out_specs=[pl.BlockSpec((rows, cols), lambda i: (0, i)) for _, _, rows in spans],
        out_shape=[jax.ShapeDtypeStruct((rows, width), jnp.bfloat16) for _, _, rows in spans],
        scratch_shapes=[pltpu.VMEM((sum(s[2] for s in spans), tok_rows), jnp.bfloat16)],
        cost_estimate=pl.CostEstimate(
            flops=2 * sum(s[2] for s in spans) * tok_rows * width,
            bytes_accessed=4 * tok_rows * width * 2,
            transcendentals=0,
        ),
        compiler_params=pltpu.CompilerParams(vmem_limit_bytes=16 << 20),
        name="more_pack",
    )(slots, normed)


def combine_kernel(spans, meta_ref, base_ref, *refs):
    rows_in, out_ref, (spread, gathered) = refs[: len(spans)], refs[len(spans)], refs[len(spans) + 1 :]

    @pl.when(pl.program_id(0) == 0)
    def _():
        lane = lax.broadcasted_iota(jnp.int32, spread.shape, 1)
        total, at = jnp.zeros(spread.shape, jnp.float32), 0
        for j, first, rows in spans:
            place = meta_ref[:, j : j + 1].astype(jnp.int32)
            inside = (place >= first) & (place < first + rows)
            target = jnp.where(inside, place - first + at, -1)
            total = jnp.where(lane == target, meta_ref[:, 4 + j : 5 + j], total)
            at += rows
        spread[...] = total.astype(jnp.bfloat16)

    at = 0
    for (j, first, rows), ref in zip(spans, rows_in):
        gathered[at : at + rows, :] = ref[...]
        at += rows
    total = base_ref[...].astype(jnp.float32) + jnp.dot(
        spread[...], gathered[...], preferred_element_type=jnp.float32
    )
    out_ref[...] = total.astype(out_ref.dtype)


def combine(meta, base, pieces, spans, tiles, dtype):
    tok_rows, width = base.shape
    cols = width // tiles
    return pl.pallas_call(
        functools.partial(combine_kernel, spans),
        grid=(tiles,),
        in_specs=[
            pl.BlockSpec(meta.shape, lambda i: (0, 0)),
            pl.BlockSpec((tok_rows, cols), lambda i: (0, i)),
        ]
        + [pl.BlockSpec((rows, cols), lambda i: (0, i)) for _, _, rows in spans],
        out_specs=pl.BlockSpec((tok_rows, cols), lambda i: (0, i)),
        out_shape=jax.ShapeDtypeStruct((tok_rows, width), dtype),
        scratch_shapes=[
            pltpu.VMEM((tok_rows, sum(s[2] for s in spans)), jnp.bfloat16),
            pltpu.VMEM((sum(s[2] for s in spans), cols), jnp.bfloat16),
        ],
        cost_estimate=pl.CostEstimate(
            flops=2 * sum(s[2] for s in spans) * tok_rows * width,
            bytes_accessed=4 * tok_rows * width * 2,
            transcendentals=0,
        ),
        compiler_params=pltpu.CompilerParams(vmem_limit_bytes=20 << 20),
        name="combine",
    )(meta, base, *pieces)


def gated_tiles(rows, gate, upper, active):
    hidden = gate.shape[1]

    def tile(at, size):
        span = pl.ds(at, size)
        g = jnp.dot(rows[...], gate[:, span], preferred_element_type=jnp.float32)
        u = jnp.dot(rows[...], upper[:, span], preferred_element_type=jnp.float32)
        active[:, span] = (g / (1.0 + jnp.exp(-g)) * u).astype(jnp.bfloat16)

    full = hidden // 256

    @pl.loop(0, full)
    def _(i):
        tile(pl.multiple_of(i * 256, 256), 256)

    if hidden % 256:
        tile(full * 256, hidden % 256)


def expert_kernel(sizes, gate_hbm, up_hbm, down_hbm, *refs):
    n = len(sizes)
    ins, outs = refs[:n], refs[n : 2 * n]
    rows, gate, upper, down, active, sems = refs[2 * n :]
    copies = [
        pltpu.make_async_copy(src, dst, sems.at[i])
        for i, (src, dst) in enumerate(((gate_hbm, gate), (up_hbm, upper), (down_hbm, down)))
    ]
    for c in copies:
        c.start()
    at = 0
    for ref, size in zip(ins, sizes):
        rows[at : at + size, :] = ref[...]
        at += size
    copies[0].wait()
    copies[1].wait()
    gated_tiles(rows, gate, upper, active)
    copies[2].wait()

    @pl.loop(0, down.shape[1] // 256)
    def _(i):
        span = pl.ds(pl.multiple_of(i * 256, 256), 256)
        result = jnp.dot(active[...], down[:, span], preferred_element_type=jnp.float32)
        result = result.astype(jnp.bfloat16)
        at = 0
        for out, size in zip(outs, sizes):
            out[:, span] = result[at : at + size]
            at += size


def expert_call(pieces, gate_weight, up_weight, down_weight):
    sizes = tuple(p.shape[0] for p in pieces)
    width, hidden = gate_weight.shape
    count = sum(sizes)
    return pl.pallas_call(
        functools.partial(expert_kernel, sizes),
        in_specs=[pl.BlockSpec(memory_space=pl.ANY)] * 3 + [pl.BlockSpec(memory_space=VMEM)] * len(sizes),
        out_specs=[pl.BlockSpec(memory_space=VMEM)] * len(sizes),
        out_shape=[jax.ShapeDtypeStruct((n, width), jnp.bfloat16) for n in sizes],
        scratch_shapes=[
            pltpu.VMEM((count, width), jnp.bfloat16),
            pltpu.VMEM((width, hidden), jnp.bfloat16),
            pltpu.VMEM((width, hidden), jnp.bfloat16),
            pltpu.VMEM((hidden, width), jnp.bfloat16),
            pltpu.VMEM((count, hidden), jnp.bfloat16),
            pltpu.SemaphoreType.DMA((3,)),
        ],
        cost_estimate=pl.CostEstimate(
            flops=6 * count * width * hidden, bytes_accessed=6 * width * hidden, transcendentals=0
        ),
        compiler_params=pltpu.CompilerParams(vmem_limit_bytes=40 << 20),
        name="expert",
    )(gate_weight, up_weight, down_weight, *pieces)


def square(
    tokens, modality, expert_ids, route_weights, norm_gain, gate_weight, up_weight, down_weight
):
    tok_rows = tokens.shape[0]
    capacity = min(tok_rows, tok_rows * expert_ids.shape[1] * 5 // 16)
    half = capacity // 2
    me = lax.axis_index("expert").astype(jnp.int32).reshape(1)
    swap = lambda value, j: lax.ppermute(value, "expert", [(i, i ^ j) for i in range(4)])
    remote = (1, 2, 3)
    spans0 = tuple((j, 0, half) for j in remote)
    spans1 = tuple((j, half, capacity - half) for j in remote)
    *out0, normed, slots, meta = first_pack(
        me, expert_ids.T, modality[None, :], route_weights.T, tokens, norm_gain, spans0, 4
    )
    got0 = [swap(v, j) for v, j in zip(out0, remote)]
    *out1, local = more_pack(slots, normed, spans1 + ((0, 0, capacity),), 4)
    got1 = [swap(v, j) for v, j in zip(out1, remote)]
    (local_out,) = expert_call([local], gate_weight, up_weight, down_weight)
    done0 = expert_call(got0, gate_weight, up_weight, down_weight)
    ret0 = [swap(v, j) for v, j in zip(done0, remote)]
    done1 = expert_call(got1, gate_weight, up_weight, down_weight)
    ret1 = [swap(v, j) for v, j in zip(done1, remote)]
    partial = combine(
        meta, tokens, [local_out] + ret0, ((0, 0, capacity),) + spans0, 4, jnp.float32
    )
    return combine(meta, partial, ret1, spans1, 4, jnp.bfloat16)


def shards(*args):
    return (square if lax.axis_size("expert") == 4 else general)(*args)


def solution(mesh):
    placed = (
        P(("dp", "expert"), None),
        P(("dp", "expert")),
        P(("dp", "expert"), None),
        P(("dp", "expert"), None),
        P(),
        P(None, "expert"),
        P(None, "expert"),
        P("expert", None),
    )
    return jax.shard_map(
        shards, mesh=mesh, in_specs=placed, out_specs=P(("dp", "expert"), None), check_vma=False
    )
```

```python
import functools
import jax
import jax.numpy as jnp
from jax import lax
from jax.experimental import pallas as pl
from jax.experimental.pallas import tpu as pltpu
from jax.sharding import PartitionSpec as P


epsilon = 1e-05
VMEM = pltpu.MemorySpace.VMEM
SMEM = pltpu.MemorySpace.SMEM


def normalize(tokens, modality, norm_gain):
    values = tokens.astype(jnp.float32)
    square = jnp.mean(values * values, axis=1, keepdims=True)
    gains = jnp.where(modality[:, None] == 1, norm_gain[1][None, :], norm_gain[0][None, :])
    return (values * lax.rsqrt(square + epsilon) * gains).astype(jnp.bfloat16)


def slot_table(expert_ids, experts, capacity):
    fanout = expert_ids.shape[1]
    flat_ids = expert_ids.reshape(-1)
    columns = jnp.arange(experts, dtype=jnp.int32)
    onehot = (flat_ids[:, None] == columns[None, :]).astype(jnp.int32)
    earlier = jnp.cumsum(onehot, axis=0) - onehot
    position = jnp.sum(earlier * onehot, axis=1)
    slots = flat_ids * capacity + position
    sources = jnp.arange(flat_ids.shape[0], dtype=jnp.int32) // fanout
    owners = jnp.full((experts * capacity,), -1, jnp.int32).at[slots].set(sources)
    return (slots, owners)


def pack_rows(normed, owners):
    chosen = jnp.take(normed, jnp.maximum(owners, 0), axis=0)
    return jnp.where(owners[:, None] >= 0, chosen, jnp.zeros_like(chosen))


def expert_rows(rows, gate_weight, up_weight, down_weight):
    gate = jnp.dot(rows, gate_weight, preferred_element_type=jnp.float32)
    upper = jnp.dot(rows, up_weight, preferred_element_type=jnp.float32)
    active = (jax.nn.silu(gate) * upper).astype(jnp.bfloat16)
    return jnp.dot(active, down_weight, preferred_element_type=jnp.float32).astype(jnp.bfloat16)


def general(
    tokens, modality, expert_ids, route_weights, norm_gain, gate_weight, up_weight, down_weight
):
    devices = lax.axis_size("expert")
    tok_rows, width = tokens.shape
    fanout = expert_ids.shape[1]
    capacity = min(tok_rows, tok_rows * fanout * 5 // (4 * devices))
    normed = normalize(tokens, modality, norm_gain)
    slots, owners = slot_table(expert_ids, devices, capacity)
    blocks = pack_rows(normed, owners).reshape(devices, capacity, width)
    arrived = lax.all_to_all(blocks, "expert", split_axis=0, concat_axis=0, tiled=True)
    finished = expert_rows(
        arrived.reshape(-1, width), gate_weight, up_weight, down_weight
    ).reshape(devices, capacity, width)
    returned = lax.all_to_all(finished, "expert", split_axis=0, concat_axis=0, tiled=True)
    expert_out = returned.reshape(devices * capacity, width)
    picked = (
        jnp.take(expert_out, slots, axis=0).reshape(tok_rows, fanout, width).astype(jnp.float32)
    )
    mixed = tokens.astype(jnp.float32) + jnp.sum(route_weights[:, :, None] * picked, axis=1)
    return mixed.astype(jnp.bfloat16)


def in_hbm(value):
    return pltpu.with_memory_space_constraint(value, pltpu.MemorySpace.HBM)


def slot_rows(slot_of, first, rows):
    want = lax.broadcasted_iota(jnp.int32, (rows, slot_of.shape[1]), 0) + first
    return jnp.where(want == slot_of, 1.0, 0.0).astype(jnp.bfloat16)


def first_pack_kernel(
    spans, me_ref, ids_hbm, mod_hbm, weight_hbm, tok_hbm, gain_hbm, *refs
):
    outs, rest = refs[: len(spans)], refs[len(spans) :]
    copy_ref, slot_ref, meta_ref, select, normed_ref = rest[:5]
    ids_ref, mod_ref, weight_ref, tok_ref, gain_ref, sems = rest[5:]
    step = pl.program_id(0)
    tok_rows = tok_ref.shape[0]
    cols = outs[0].shape[1]

    @pl.when(step == 0)
    def _():
        pairs = ((ids_hbm, ids_ref), (mod_hbm, mod_ref), (weight_hbm, weight_ref))
        pairs += ((gain_hbm, gain_ref), (tok_hbm, tok_ref))
        copies = [pltpu.make_async_copy(x, y, sems.at[i]) for i, (x, y) in enumerate(pairs)]
        for c in copies:
            c.start()
        for c in copies[:-1]:
            c.wait()
        ids = ids_ref[...]
        rank = lax.broadcasted_iota(jnp.int32, (8, tok_rows), 0)
        wanted = jnp.bitwise_xor(rank, me_ref[0])
        hit0, hit1 = wanted == ids[0:1, :], wanted == ids[1:2, :]
        member = jnp.where((hit0 | hit1) & (rank < 4), 1.0, 0.0)
        weight = jnp.where(hit0, weight_ref[0:1, :], jnp.where(hit1, weight_ref[1:2, :], 0.0))
        before = lax.broadcasted_iota(jnp.int32, (tok_rows, tok_rows), 0) < lax.broadcasted_iota(
            jnp.int32, (tok_rows, tok_rows), 1
        )
        earlier = jnp.dot(
            member.astype(jnp.bfloat16),
            jnp.where(before, 1.0, 0.0).astype(jnp.bfloat16),
            preferred_element_type=jnp.float32,
        )
        place = jnp.where(member > 0, earlier, -1.0)
        slot_ref[...] = place.astype(jnp.int32)
        packed = jnp.concatenate([place[0:4], weight[0:4]], axis=0)
        meta_ref[...] = jnp.concatenate(
            [packed, jnp.zeros((120, tok_rows), jnp.float32)], axis=0
        ).T
        image = jnp.concatenate(
            [mod_ref[...].astype(jnp.float32), jnp.zeros((127, tok_rows), jnp.float32)], axis=0
        ).T[:, 0:1]
        copies[-1].wait()
        for lo in range(0, tok_rows, 64):
            values = tok_ref[lo : lo + 64, :].astype(jnp.float32)
            square = jnp.mean(values * values, axis=1, keepdims=True)
            gains = jnp.where(image[lo : lo + 64] > 0.5, gain_ref[1:2, :], gain_ref[0:1, :])
            normed_ref[lo : lo + 64, :] = (
                values * lax.rsqrt(square + epsilon) * gains
            ).astype(jnp.bfloat16)
        base = 0
        for j, first, rows in spans:
            select[base : base + rows, :] = slot_rows(place[j : j + 1, :].astype(jnp.int32), first, rows)
            base += rows

    base = 0
    at = pl.ds(pl.multiple_of(step * cols, cols), cols)
    part = normed_ref[:, at]
    copy_ref[...] = part
    chosen = jnp.dot(select[...], part, preferred_element_type=jnp.float32).astype(jnp.bfloat16)
    for out, (j, first, rows) in zip(outs, spans):
        out[...] = chosen[base : base + rows]
        base += rows


def first_pack(me, ids_t, mod, weight_t, tokens, gain, spans, tiles):
    tok_rows, width = tokens.shape
    cols = width // tiles
    whole = lambda *shape: pl.BlockSpec(shape, lambda i: (0,) * len(shape))
    return pl.pallas_call(
        functools.partial(first_pack_kernel, spans),
        grid=(tiles,),
        in_specs=[
            pl.BlockSpec(memory_space=SMEM),
        ]
        + [pl.BlockSpec(memory_space=pltpu.MemorySpace.HBM)] * 5,
        out_specs=[pl.BlockSpec((rows, cols), lambda i: (0, i)) for _, _, rows in spans]
        + [pl.BlockSpec((tok_rows, cols), lambda i: (0, i)), whole(8, tok_rows), whole(tok_rows, 128)],
        out_shape=[jax.ShapeDtypeStruct((rows, width), jnp.bfloat16) for _, _, rows in spans]
        + [
            jax.ShapeDtypeStruct((tok_rows, width), jnp.bfloat16),
            jax.ShapeDtypeStruct((8, tok_rows), jnp.int32),
            jax.ShapeDtypeStruct((tok_rows, 128), jnp.float32),
        ],
        scratch_shapes=[
            pltpu.VMEM((sum(s[2] for s in spans), tok_rows), jnp.bfloat16),
            pltpu.VMEM((tok_rows, width), jnp.bfloat16),
            pltpu.VMEM(ids_t.shape, ids_t.dtype),
            pltpu.VMEM(mod.shape, mod.dtype),
            pltpu.VMEM(weight_t.shape, weight_t.dtype),
            pltpu.VMEM(tokens.shape, tokens.dtype),
            pltpu.VMEM(gain.shape, gain.dtype),
            pltpu.SemaphoreType.DMA((5,)),
        ],
        cost_estimate=pl.CostEstimate(
            flops=2 * sum(s[2] for s in spans) * tok_rows * width,
            bytes_accessed=4 * tok_rows * width * 2,
            transcendentals=0,
        ),
        compiler_params=pltpu.CompilerParams(vmem_limit_bytes=16 << 20),
        name="first_pack",
    )(me, *(in_hbm(v) for v in (ids_t, mod, weight_t, tokens, gain)))


def more_pack_kernel(spans, slot_ref, normed_ref, *refs):
    outs, select = refs[:-1], refs[-1]

    @pl.when(pl.program_id(0) == 0)
    def _():
        base = 0
        for j, first, rows in spans:
            select[base : base + rows, :] = slot_rows(slot_ref[j : j + 1, :], first, rows)
            base += rows

    chosen = jnp.dot(select[...], normed_ref[...], preferred_element_type=jnp.float32).astype(jnp.bfloat16)
    base = 0
    for out, (j, first, rows) in zip(outs, spans):
        out[...] = chosen[base : base + rows]
        base += rows


def more_pack(slots, normed, spans, tiles):
    tok_rows, width = normed.shape
    cols = width // tiles
    return pl.pallas_call(
        functools.partial(more_pack_kernel, spans),
        grid=(tiles,),
        in_specs=[
            pl.BlockSpec(slots.shape, lambda i: (0, 0)),
            pl.BlockSpec((tok_rows, cols), lambda i: (0, i)),
        ],
        out_specs=[pl.BlockSpec((rows, cols), lambda i: (0, i)) for _, _, rows in spans],
        out_shape=[jax.ShapeDtypeStruct((rows, width), jnp.bfloat16) for _, _, rows in spans],
        scratch_shapes=[pltpu.VMEM((sum(s[2] for s in spans), tok_rows), jnp.bfloat16)],
        cost_estimate=pl.CostEstimate(
            flops=2 * sum(s[2] for s in spans) * tok_rows * width,
            bytes_accessed=4 * tok_rows * width * 2,
            transcendentals=0,
        ),
        compiler_params=pltpu.CompilerParams(vmem_limit_bytes=16 << 20),
        name="more_pack",
    )(slots, normed)


def combine_kernel(spans, meta_ref, base_ref, *refs):
    rows_in, out_ref, (spread, gathered) = refs[: len(spans)], refs[len(spans)], refs[len(spans) + 1 :]

    @pl.when(pl.program_id(0) == 0)
    def _():
        lane = lax.broadcasted_iota(jnp.int32, spread.shape, 1)
        total, at = jnp.zeros(spread.shape, jnp.float32), 0
        for j, first, rows in spans:
            place = meta_ref[:, j : j + 1].astype(jnp.int32)
            inside = (place >= first) & (place < first + rows)
            target = jnp.where(inside, place - first + at, -1)
            total = jnp.where(lane == target, meta_ref[:, 4 + j : 5 + j], total)
            at += rows
        spread[...] = total.astype(jnp.bfloat16)

    at = 0
    for (j, first, rows), ref in zip(spans, rows_in):
        gathered[at : at + rows, :] = ref[...]
        at += rows
    total = base_ref[...].astype(jnp.float32) + jnp.dot(
        spread[...], gathered[...], preferred_element_type=jnp.float32
    )
    out_ref[...] = total.astype(out_ref.dtype)


def combine(meta, base, pieces, spans, tiles, dtype):
    tok_rows, width = base.shape
    cols = width // tiles
    return pl.pallas_call(
        functools.partial(combine_kernel, spans),
        grid=(tiles,),
        in_specs=[
            pl.BlockSpec(meta.shape, lambda i: (0, 0)),
            pl.BlockSpec((tok_rows, cols), lambda i: (0, i)),
        ]
        + [pl.BlockSpec((rows, cols), lambda i: (0, i)) for _, _, rows in spans],
        out_specs=pl.BlockSpec((tok_rows, cols), lambda i: (0, i)),
        out_shape=jax.ShapeDtypeStruct((tok_rows, width), dtype),
        scratch_shapes=[
            pltpu.VMEM((tok_rows, sum(s[2] for s in spans)), jnp.bfloat16),
            pltpu.VMEM((sum(s[2] for s in spans), cols), jnp.bfloat16),
        ],
        cost_estimate=pl.CostEstimate(
            flops=2 * sum(s[2] for s in spans) * tok_rows * width,
            bytes_accessed=4 * tok_rows * width * 2,
            transcendentals=0,
        ),
        compiler_params=pltpu.CompilerParams(vmem_limit_bytes=20 << 20),
        name="combine",
    )(meta, base, *pieces)


def gated_tiles(rows, gate, upper, active):
    hidden = gate.shape[1]

    def tile(at, size):
        span = pl.ds(at, size)
        g = jnp.dot(rows[...], gate[:, span], preferred_element_type=jnp.float32)
        u = jnp.dot(rows[...], upper[:, span], preferred_element_type=jnp.float32)
        active[:, span] = (g / (1.0 + jnp.exp(-g)) * u).astype(jnp.bfloat16)

    full = hidden // 256

    @pl.loop(0, full)
    def _(i):
        tile(pl.multiple_of(i * 256, 256), 256)

    if hidden % 256:
        tile(full * 256, hidden % 256)


def expert_kernel(sizes, gate_hbm, up_hbm, down_hbm, *refs):
    n = len(sizes)
    ins, outs = refs[:n], refs[n : 2 * n]
    rows, gate, upper, down, active, sems = refs[2 * n :]
    copies = [
        pltpu.make_async_copy(src, dst, sems.at[i])
        for i, (src, dst) in enumerate(((gate_hbm, gate), (up_hbm, upper), (down_hbm, down)))
    ]
    for c in copies:
        c.start()
    at = 0
    for ref, size in zip(ins, sizes):
        rows[at : at + size, :] = ref[...]
        at += size
    copies[0].wait()
    copies[1].wait()
    gated_tiles(rows, gate, upper, active)
    copies[2].wait()

    @pl.loop(0, down.shape[1] // 256)
    def _(i):
        span = pl.ds(pl.multiple_of(i * 256, 256), 256)
        result = jnp.dot(active[...], down[:, span], preferred_element_type=jnp.float32)
        result = result.astype(jnp.bfloat16)
        at = 0
        for out, size in zip(outs, sizes):
            out[:, span] = result[at : at + size]
            at += size


def expert_call(pieces, gate_weight, up_weight, down_weight):
    sizes = tuple(p.shape[0] for p in pieces)
    width, hidden = gate_weight.shape
    count = sum(sizes)
    return pl.pallas_call(
        functools.partial(expert_kernel, sizes),
        in_specs=[pl.BlockSpec(memory_space=pl.ANY)] * 3 + [pl.BlockSpec(memory_space=VMEM)] * len(sizes),
        out_specs=[pl.BlockSpec(memory_space=VMEM)] * len(sizes),
        out_shape=[jax.ShapeDtypeStruct((n, width), jnp.bfloat16) for n in sizes],
        scratch_shapes=[
            pltpu.VMEM((count, width), jnp.bfloat16),
            pltpu.VMEM((width, hidden), jnp.bfloat16),
            pltpu.VMEM((width, hidden), jnp.bfloat16),
            pltpu.VMEM((hidden, width), jnp.bfloat16),
            pltpu.VMEM((count, hidden), jnp.bfloat16),
            pltpu.SemaphoreType.DMA((3,)),
        ],
        cost_estimate=pl.CostEstimate(
            flops=6 * count * width * hidden, bytes_accessed=6 * width * hidden, transcendentals=0
        ),
        compiler_params=pltpu.CompilerParams(vmem_limit_bytes=40 << 20),
        name="expert",
    )(*(in_hbm(v) for v in (gate_weight, up_weight, down_weight)), *pieces)


def square(
    tokens, modality, expert_ids, route_weights, norm_gain, gate_weight, up_weight, down_weight
):
    tok_rows = tokens.shape[0]
    capacity = min(tok_rows, tok_rows * expert_ids.shape[1] * 5 // 16)
    half = capacity // 2
    me = lax.axis_index("expert").astype(jnp.int32).reshape(1)
    swap = lambda value, j: lax.ppermute(value, "expert", [(i, i ^ j) for i in range(4)])
    remote = (1, 2, 3)
    spans0 = tuple((j, 0, half) for j in remote)
    spans1 = tuple((j, half, capacity - half) for j in remote)
    *out0, normed, slots, meta = first_pack(
        me, expert_ids.T, modality[None, :], route_weights.T, tokens, norm_gain, spans0, 4
    )
    got0 = [swap(v, j) for v, j in zip(out0, remote)]
    *out1, local = more_pack(slots, normed, spans1 + ((0, 0, capacity),), 4)
    got1 = [swap(v, j) for v, j in zip(out1, remote)]
    (local_out,) = expert_call([local], gate_weight, up_weight, down_weight)
    done0 = expert_call(got0, gate_weight, up_weight, down_weight)
    ret0 = [swap(v, j) for v, j in zip(done0, remote)]
    done1 = expert_call(got1, gate_weight, up_weight, down_weight)
    ret1 = [swap(v, j) for v, j in zip(done1, remote)]
    partial = combine(
        meta, tokens, [local_out] + ret0, ((0, 0, capacity),) + spans0, 4, jnp.float32
    )
    return combine(meta, partial, ret1, spans1, 4, jnp.bfloat16)


def shards(*args):
    return (square if lax.axis_size("expert") == 4 else general)(*args)


def solution(mesh):
    placed = (
        P(("dp", "expert"), None),
        P(("dp", "expert")),
        P(("dp", "expert"), None),
        P(("dp", "expert"), None),
        P(),
        P(None, "expert"),
        P(None, "expert"),
        P("expert", None),
    )
    return jax.shard_map(
        shards, mesh=mesh, in_specs=placed, out_specs=P(("dp", "expert"), None), check_vma=False
    )
```
